32 devices in a mesh: aa: 8 (over z, x), ba: 4 (over y, core).
Axes of the slice: x: 2, y: 2, z: 4, core: 2. Of those that a mesh axis runs over, the one named last changes fastest.
Arguments:
- grid_features: bfloat16 [128, 128, 256, 128], P('aa', 'ba'), may hold values from -6 to 6
- weight_real: bfloat16 [32, 32, 16, 128, 128], P('ba', None, 'aa'), may hold values from -6 to 6
- weight_imag: bfloat16 [32, 32, 16, 128, 128], P('ba', None, 'aa'), may hold values from -6 to 6
- mode_keep: int32 [32, 16], P('ba', 'aa'), may hold values from 1 to 16, as said below
- local_weight: bfloat16 [128, 128], replicated, may hold values from -0.5 to 0.5
- local_bias: bfloat16 [128], replicated, may hold values from -3 to 3
Outputs:
- layer_output: bfloat16 [128, 128, 256, 128], P('aa', 'ba')
The draws below stay inside these ranges and needn't reach their ends.
Inputs may be any that keep to these rules, and one draw needn't show every extreme that they name: mode_keep[i, k] counts the retained levels of the second frequency on the line of the i-th retained first frequency and the k-th third frequency.
All inputs are finite; a program needn't handle non-finite values.
Results may differ from the reference program's by a relative error of at most 0.012.
Values may be sent and summed in bfloat16 or wider, within the bound.
A program may use at most 256 MiB of HBM per device.

```python
import math
import jax
import jax.numpy as jnp
from jax import lax

NX = 128
NY = 128
NZ = 256
C = 128
KX = 32
KY = 32
KZ = 16
N_AA = 8


def draw_mode_keep(key, part):
    top_level = KY // 2
    positions = jnp.arange(KX, dtype=jnp.int32)
    level_first = jnp.where(positions < KX // 2, positions, KX - 1 - positions)
    level_third = jnp.arange(KZ, dtype=jnp.int32)
    reach_total = KX // 2 + KZ
    base_level = top_level - (level_first[:, None] + level_third[None, :]) * top_level // reach_total
    jitter = jax.random.randint(key, (KX, KZ), -3, 4, dtype=jnp.int32)
    kept_levels = jnp.clip(base_level + jitter, 1, top_level)
    kept_levels = kept_levels.at[0, 0].set(top_level)
    kept_levels = kept_levels.at[KX // 2 - 1, KZ - 1].set(1)
    return kept_levels.astype(jnp.int32)


def block_levels(own_key, dims, shards, low, top_value):
    def one(dim, shards_of):
        draws = jax.random.uniform(jax.random.fold_in(jax.random.fold_in(own_key, 6), dim), (shards_of,), jnp.float32, low / len(shards), top_value / len(shards))
        return jnp.repeat(jnp.exp(draws), dims[dim] // shards_of).reshape((-1,) + (1,) * (len(dims) - dim - 1))

    gain = one(*shards[0])
    for cut in shards[1:]:
        gain = gain * one(*cut)
    return gain


def centred(rng, extent, spread, limit, pieces=(), kind=jnp.bfloat16):
    drawn = jax.random.normal(rng, extent, jnp.float32) * spread
    if len(pieces) > 0:
        drawn = block_levels(rng, extent, pieces, -0.22, 0.18) * drawn
    return jnp.clip(drawn, min=-limit, max=limit).astype(kind)


def setup_inputs(seed: int = 0) -> dict:
    keys = jax.random.split(jax.random.key(seed), 7)
    grid_features = centred(keys[0], (NX, NY, NZ, C), 1.0, 6.0, ((0, 8), (1, 4)))
    weight_real = centred(keys[1], (KX, KY, KZ, C, C), 1.0, 6.0, ((0, 4), (2, 8)))
    weight_imag = centred(keys[2], (KX, KY, KZ, C, C), 1.0, 6.0, ((0, 4), (2, 8)))
    mode_keep = draw_mode_keep(jax.random.fold_in(keys[6], 71), 0)
    local_weight = centred(keys[4], (C, C), C ** -0.5, 0.5)
    local_bias = centred(keys[5], (C,), 0.5, 3.0)
    return {"grid_features": grid_features, "weight_real": weight_real, "weight_imag": weight_imag, "mode_keep": mode_keep, "local_weight": local_weight, "local_bias": local_bias}


highest = lax.Precision.HIGHEST


def kept_modes(length, number):
    positions = jnp.arange(number, dtype=jnp.int32)
    return jnp.where(positions < number // 2, positions, positions + (length - number)).astype(jnp.int32)


def phase_tables(length, mode_list):
    places = jnp.arange(length, dtype=jnp.int32)
    phase_steps = (places[:, None] * mode_list[None, :]) % length
    angles = phase_steps.astype(jnp.float32) * (2.0 * math.pi / length)
    return jnp.cos(angles), jnp.sin(angles)


def forward_kernel(length, number):
    cosine_table, sine_table = phase_tables(length, kept_modes(length, number))
    upper_rows = jnp.concatenate([cosine_table, -sine_table], axis=1)
    lower_rows = jnp.concatenate([sine_table, cosine_table], axis=1)
    return jnp.concatenate([upper_rows, lower_rows], axis=0)


def inverse_kernel(length, number):
    cosine_table, sine_table = phase_tables(length, kept_modes(length, number))
    upper_rows = jnp.concatenate([cosine_table.T, sine_table.T], axis=1)
    lower_rows = jnp.concatenate([-sine_table.T, cosine_table.T], axis=1)
    return jnp.concatenate([upper_rows, lower_rows], axis=0)


def depth_kernels():
    cosine_table, sine_table = phase_tables(NZ, jnp.arange(KZ, dtype=jnp.int32))
    forward = jnp.concatenate([cosine_table, -sine_table], axis=1).astype(jnp.bfloat16)
    factor = jnp.where(jnp.arange(KZ, dtype=jnp.int32) == 0, 1.0, 2.0).astype(jnp.float32) / (NX * NY * NZ)
    inverse = jnp.concatenate([cosine_table.T * factor[:, None], -sine_table.T * factor[:, None]], axis=0).astype(jnp.bfloat16)
    return forward, inverse


def along_first(operand, kernel):
    return jnp.einsum('pabc,pq->qabc', operand, kernel, precision=highest, preferred_element_type=jnp.float32)


def along_second(operand, kernel):
    return jnp.einsum('apbc,pq->aqbc', operand, kernel, precision=highest, preferred_element_type=jnp.float32)


def mode_mask(kept_counts):
    positions = jnp.arange(KY, dtype=jnp.int32)
    levels = jnp.where(positions < KY // 2, positions, KY - 1 - positions)
    return (levels[None, :, None] < kept_counts[:, None, :]).astype(jnp.float32)


def reference(grid_features, weight_real, weight_imag, mode_keep, local_weight, local_bias):
    forward_depth, inverse_depth = depth_kernels()
    slab_rows = NX // N_AA
    field_slabs = grid_features.reshape(N_AA, slab_rows, NY, NZ, C)

    def depth_forward(slab_cells):
        flat_rows = jnp.transpose(slab_cells, (0, 1, 3, 2)).reshape(slab_rows * NY * C, NZ).astype(jnp.float32)
        coeffs = jnp.dot(flat_rows, forward_depth.astype(jnp.float32), precision=highest, preferred_element_type=jnp.float32)
        coeffs = jnp.transpose(coeffs.reshape(slab_rows, NY, C, 2 * KZ), (0, 1, 3, 2))
        return coeffs.astype(jnp.bfloat16)

    coeffs = lax.map(depth_forward, field_slabs).reshape(NX, NY, 2 * KZ, C)
    stacked = jnp.concatenate([coeffs[:, :, :KZ], coeffs[:, :, KZ:]], axis=0).astype(jnp.float32)
    result = along_first(stacked, forward_kernel(NX, KX))
    result = jnp.concatenate([result[:KX], result[KX:]], axis=1)
    result = along_second(result, forward_kernel(NY, KY)).astype(jnp.bfloat16)
    spec_real = result[:, :KY]
    spec_imag = result[:, KY:]

    def mix_line(operands):
        real_part, imag_part, line_real, line_imag = operands
        real_part = real_part.astype(jnp.float32)
        imag_part = imag_part.astype(jnp.float32)
        line_real = line_real.astype(jnp.float32)
        line_imag = line_imag.astype(jnp.float32)
        pattern = 'bcd,bcde->bce'
        out_real = jnp.einsum(pattern, real_part, line_real, precision=highest) - jnp.einsum(pattern, imag_part, line_imag, precision=highest)
        out_imag = jnp.einsum(pattern, real_part, line_imag, precision=highest) + jnp.einsum(pattern, imag_part, line_real, precision=highest)
        return out_real, out_imag

    mixed_real, mixed_imag = lax.map(mix_line, (spec_real, spec_imag, weight_real, weight_imag))
    keep_mask = mode_mask(mode_keep)[..., None]
    mixed_real = mixed_real * keep_mask
    mixed_imag = mixed_imag * keep_mask
    result = along_second(jnp.concatenate([mixed_real, mixed_imag], axis=1), inverse_kernel(NY, KY))
    result = jnp.concatenate([result[:, :NY], result[:, NY:]], axis=0)
    result = along_first(result, inverse_kernel(NX, KX)).astype(jnp.bfloat16)
    back_field = jnp.concatenate([result[:NX], result[NX:]], axis=2)
    back_slabs = back_field.reshape(N_AA, slab_rows, NY, 2 * KZ, C)

    def finish_slab(operands):
        slab_cells, back_slab = operands
        flat_rows = jnp.transpose(back_slab, (0, 1, 3, 2)).reshape(slab_rows * NY * C, 2 * KZ).astype(jnp.float32)
        spectral = jnp.dot(flat_rows, inverse_depth.astype(jnp.float32), precision=highest, preferred_element_type=jnp.float32)
        spectral = jnp.transpose(spectral.reshape(slab_rows, NY, C, NZ), (0, 1, 3, 2))
        local_term = jnp.dot(slab_cells.reshape(-1, C).astype(jnp.float32), local_weight.astype(jnp.float32), precision=highest, preferred_element_type=jnp.float32)
        local_term = local_term.reshape(slab_rows, NY, NZ, C)
        return jax.nn.gelu(spectral + local_term + local_bias.astype(jnp.float32)).astype(jnp.bfloat16)

    return lax.map(finish_slab, (field_slabs, back_slabs)).reshape(NX, NY, NZ, C)
```

```python
import functools
import math

import jax
import jax.numpy as jnp
import numpy as np
from jax import lax
from jax.experimental import pallas as pl
from jax.experimental.pallas import tpu as pltpu
from jax.sharding import PartitionSpec as P

BF = jnp.bfloat16
F32 = jnp.float32
MESH = pl.DeviceIdType.MESH


def kept_modes(length, number, positions):
    return np.where(positions < number // 2, positions, positions + (length - number))


def phase_tables(length, places, mode_list):
    phase_steps = places[:, None] * mode_list[None, :] % length
    angles = phase_steps.astype(np.float32) * np.float32(2.0 * math.pi / length)
    return np.cos(angles), np.sin(angles)


def forward_table(length, places, modes):
    c, s = phase_tables(length, places, modes)
    return np.stack([np.stack([c, -s], 1), np.stack([s, c], 1)], 0)


def inverse_table(length, places, modes):
    c, s = phase_tables(length, places, modes)
    c, s = c.T, s.T
    return np.stack([np.stack([c, s], 1), np.stack([-s, c], 1)], 0)


def spectral_body(
    n_aa, n_ba, halves, parts, slots,
    depth_ref, y_ref, x_fwd_ref, x_inv_ref, keep_ref, x_ref, wr_ref, wi_ref,
    out_ref,
    xbuf, wbuf, lines, plane, sends, gots, outgo, landed, spec_out, spec_in,
    mix_out, mix_in, back,
    x_sem, w_sem, rs_send, rs_recv, fa_send, fa_recv, ba_send, ba_recv,
    ia_send, ia_recv, ag_send, ag_recv,
):
    n_x, n_y, depth, chans = x_ref.shape
    kx_own, ky, kz_own = wr_ref.shape[:3]
    kz = kz_own * n_aa
    ky_own = ky // n_ba
    q_part = ky_own // parts
    bits = n_ba.bit_length() - 1
    x_half = n_x // halves
    rows2 = 2 * x_half
    me_a = lax.axis_index("aa")
    me_b = lax.axis_index("ba")

    barrier = pltpu.get_barrier_semaphore()
    for d in range(1, n_aa):
        pl.semaphore_signal(barrier, inc=1, device_id=((me_a + d) % n_aa, me_b), device_id_type=MESH)
    for d in range(1, n_ba):
        pl.semaphore_signal(barrier, inc=1, device_id=(me_a, (me_b + d) % n_ba), device_id_type=MESH)

    def fetch(i):
        return pltpu.make_async_copy(x_ref.at[i], xbuf.at[i % slots], x_sem.at[i % slots])

    for i in range(slots):
        fetch(i).start()

    stride = lines.shape[0] // (2 * kz)

    def row(i, carry):
        fetch(i).wait()
        slot = i % slots
        for j in range(0, n_y, 2):
            pair = jnp.concatenate([xbuf[slot, j], xbuf[slot, j + 1]], axis=1)
            res = jnp.dot(depth_ref[...], pair, preferred_element_type=F32)
            for u in range(2):
                for g in range(2 * kz // 8):
                    lines[pl.ds(8 * g * stride + j + u, 8, stride=stride), :] = res[
                        8 * g : 8 * g + 8, u * chans : (u + 1) * chans
                    ]

        @pl.when(i + slots < n_x)
        def _():
            fetch(i + slots).start()

        half = i // x_half
        local = i % x_half
        for k in range(0, kz, 2):
            cols = []
            for kk in (k, k + 1):
                re = lines[kk * stride : kk * stride + n_y, :]
                im = lines[(kz + kk) * stride : (kz + kk) * stride + n_y, :]
                cols.append(jnp.concatenate([re, im], axis=0).astype(BF))
            res = jnp.dot(y_ref[...], jnp.concatenate(cols, axis=1), preferred_element_type=F32)
            for u in range(2):
                for g in range(2 * ky // 8):
                    start = (k + u) * 2 * ky * x_half + 8 * g * x_half + local
                    plane[half, pl.ds(start, 8, stride=x_half), :] = res[
                        8 * g : 8 * g + 8, u * chans : (u + 1) * chans
                    ]
        return carry

    def partner(bit):
        return (me_a, me_b ^ (1 << bit))

    def chunk_sum(h, c, blk, k, q, upto):
        base = ((k * n_ba + blk) * parts + c) * q_part + q
        total = plane[h, pl.ds(base * rows2, rows2), :]
        for t in range(upto):
            total = total + gots[t][h * parts + c, blk, k, q].astype(F32)
        return total

    def rs_copy(s, g):
        return pltpu.make_async_remote_copy(
            src_ref=sends[s].at[g], dst_ref=gots[s].at[g],
            send_sem=rs_send.at[s, g], recv_sem=rs_recv.at[s, g],
            device_id=partner(s), device_id_type=MESH,
        )

    def rs_step(s, h, c):
        g = h * parts + c
        if s > 0:
            rs_copy(s - 1, g).wait_recv()
        left = n_ba >> (s + 1)

        def one(k, carry):
            for blk in range(left):
                for q in range(q_part):
                    sends[s][g, blk, k, q] = chunk_sum(h, c, left + blk, k, q, s).astype(BF)
            return carry

        lax.fori_loop(0, kz, one, 0)
        rs_copy(s, g).start()

    def fa_copy(g, d):
        peer = (me_a + d) % n_aa
        return pltpu.make_async_remote_copy(
            src_ref=outgo.at[g, peer], dst_ref=landed.at[g, me_a],
            send_sem=fa_send.at[g, d], recv_sem=fa_recv.at[g, d],
            device_id=(peer, me_b), device_id_type=MESH,
        )

    def fa_step(h, c):
        g = h * parts + c
        rs_copy(bits - 1, g).wait_recv()

        def one(a, carry):
            for kk in range(kz_own):
                for q in range(q_part):
                    outgo[g, a, kk, q] = chunk_sum(h, c, 0, a * kz_own + kk, q, bits).astype(BF)
            return carry

        lax.fori_loop(0, n_aa, one, 0)
        for d in range(1, n_aa):
            fa_copy(g, d).start()
        landed[g, me_a] = outgo[g, me_a]

    def weight_fetch(p, m):
        ref = (wr_ref, wi_ref)[p]
        return pltpu.make_async_copy(ref.at[m], wbuf.at[p, m], w_sem.at[p, m])

    everything = [(h, c) for h in range(halves) for c in range(parts)]

    lax.fori_loop(0, x_half, row, 0)
    pl.semaphore_wait(barrier, n_aa + n_ba - 2)
    for c in range(parts):
        rs_step(0, 0, c)
    for h in range(1, halves):
        first = h * x_half
        lax.fori_loop(first, first + 2, row, 0)
        for c in range(parts):
            rs_step(1, h - 1, c)
        lax.fori_loop(first + 2, first + x_half, row, 0)
        for c in range(parts):
            rs_step(0, h, c)
    for p in range(2):
        for m in range(kx_own):
            weight_fetch(p, m).start()
    for s in range(1, bits):
        for h, c in everything:
            if s > 1 or h == halves - 1:
                rs_step(s, h, c)
    for h, c in everything:
        fa_step(h, c)

    def ba_copy(which, d):
        peer = (me_b + d) % n_ba
        src, dst = ((spec_out, spec_in), (mix_out, mix_in))[which]
        return pltpu.make_async_remote_copy(
            src_ref=src.at[peer], dst_ref=dst.at[me_b],
            send_sem=ba_send.at[which, d], recv_sem=ba_recv.at[which, d],
            device_id=(me_a, peer), device_id_type=MESH,
        )

    own2 = 2 * kx_own
    for c in range(parts):
        for h in range(halves):
            for d in range(1, n_aa):
                fa_copy(h * parts + c, d).wait_recv()
        for kk in range(kz_own):
            for q in range(0, q_part, 2):
                cols = []
                for qq in (q, q + 1):
                    cols.append(jnp.concatenate(
                        [landed[h * parts + c, a, kk, qq] for h in range(halves) for a in range(n_aa)], axis=0
                    ))
                res = jnp.dot(x_fwd_ref[...], jnp.concatenate(cols, axis=1), preferred_element_type=F32)
                for u in range(2):
                    for b in range(n_ba):
                        spec_out[b, kk, c * q_part + q + u] = res[
                            b * own2 : (b + 1) * own2, u * chans : (u + 1) * chans
                        ].astype(BF)
    for d in range(1, n_ba):
        ba_copy(0, d).start()
    spec_in[me_b] = spec_out[me_b]
    for p in range(2):
        for m in range(kx_own):
            weight_fetch(p, m).wait()
    for d in range(1, n_ba):
        ba_copy(0, d).wait_recv()

    place = lax.broadcasted_iota(jnp.int32, (own2, chans), 0) % kx_own

    def mix(j, carry):
        b = j // ky_own
        q = j % ky_own
        level = jnp.where(j < ky // 2, j, ky - 1 - j)
        for kk in range(kz_own):
            val = spec_in[b, kk, q].astype(F32)
            turned = jnp.concatenate([-val[kx_own:], val[:kx_own]], axis=0)
            lhs = jnp.concatenate([val, turned], axis=1).astype(BF)
            total = jnp.zeros((own2, chans), F32)
            for m in range(0, kx_own, 2):
                cols = [
                    jnp.concatenate([wbuf[0, mm, j, kk], wbuf[1, mm, j, kk]], axis=0) for mm in (m, m + 1)
                ]
                res = jnp.dot(lhs, jnp.concatenate(cols, axis=1), preferred_element_type=F32)
                total = jnp.where(place == m, res[:, :chans], total)
                total = jnp.where(place == m + 1, res[:, chans:], total)
            total = jnp.where(level < keep_ref[kk], total, 0.0)
            mix_out[b, q, kk] = total.astype(BF)
        return carry

    lax.fori_loop(0, ky, mix, 0)
    for d in range(1, n_ba):
        ba_copy(1, d).start()
    mix_in[me_b] = mix_out[me_b]
    for d in range(1, n_ba):
        ba_copy(1, d).wait_recv()

    def ia_copy(g, d):
        peer = (me_a + d) % n_aa
        return pltpu.make_async_remote_copy(
            src_ref=back.at[g, peer], dst_ref=out_ref.at[g, 0, me_a],
            send_sem=ia_send.at[g, d], recv_sem=ia_recv.at[g, d],
            device_id=(peer, me_b), device_id_type=MESH,
        )

    for c in range(parts):
        for kk in range(kz_own):
            for q in range(0, q_part, 2):
                cols = []
                for qq in (c * q_part + q, c * q_part + q + 1):
                    cols.append(jnp.concatenate(
                        [mix_in[b, qq, kk].astype(F32) for b in range(n_ba)], axis=0
                    ).astype(BF))
                res = jnp.dot(x_inv_ref[...], jnp.concatenate(cols, axis=1), preferred_element_type=F32)
                for u in range(2):
                    for h in range(halves):
                        for a in range(n_aa):
                            first = (h * n_aa + a) * rows2
                            back[h * parts + c, a, kk, q + u] = res[
                                first : first + rows2, u * chans : (u + 1) * chans
                            ].astype(BF)
        for h in range(halves):
            for d in range(1, n_aa):
                ia_copy(h * parts + c, d).start()
            out_ref[h * parts + c, 0, me_a] = back[h * parts + c, me_a]

    order = [h * parts + c for c in range(parts) for h in range(halves)]

    def ag_copy(t, g):
        n = 1 << (bits - 1 - t)
        return pltpu.make_async_remote_copy(
            src_ref=out_ref.at[g, pl.ds(0, n)], dst_ref=out_ref.at[g, pl.ds(n, n)],
            send_sem=ag_send.at[t, g], recv_sem=ag_recv.at[t, g],
            device_id=partner(t), device_id_type=MESH,
        )

    steps = list(reversed(range(bits)))
    total_chunks = len(order)
    for tick in range(total_chunks + bits - 1):
        for n, t in enumerate(steps):
            pos = tick - n
            if 0 <= pos < total_chunks:
                g = order[pos]
                if n == 0:
                    for d in range(1, n_aa):
                        ia_copy(g, d).wait_recv()
                else:
                    ag_copy(steps[n - 1], g).wait_recv()
                ag_copy(t, g).start()
    for g in order:
        ag_copy(steps[-1], g).wait_recv()

    for g in range(halves * parts):
        for s in range(bits):
            rs_copy(s, g).wait_send()
            ag_copy(s, g).wait_send()
        for d in range(1, n_aa):
            fa_copy(g, d).wait_send()
            ia_copy(g, d).wait_send()
    for which in range(2):
        for d in range(1, n_ba):
            ba_copy(which, d).wait_send()


def spectral(n_aa, n_ba, halves, parts, grid_features, weight_real, weight_imag, tables):
    n_x, n_y, depth, chans = grid_features.shape
    kx_own, ky, kz_own = weight_real.shape[:3]
    kz = kz_own * n_aa
    ky_own = ky // n_ba
    q_part = ky_own // parts
    bits = n_ba.bit_length() - 1
    rows2 = 2 * n_x // halves
    chunks = halves * parts
    slots = 4
    stride = n_y + 8
    vm = pltpu.VMEM
    dma = pltpu.SemaphoreType.DMA

    def rs_shape(s):
        left = n_ba >> (s + 1)
        return vm((chunks, left, kz, q_part, rows2, chans), BF)

    inner = pl.BlockSpec(memory_space=pltpu.VMEM)
    outer = pl.BlockSpec(memory_space=pl.ANY)
    return pl.pallas_call(
        functools.partial(spectral_body, n_aa, n_ba, halves, parts, slots),
        in_specs=[inner] * 5 + [outer] * 3,
        out_specs=inner,
        out_shape=jax.ShapeDtypeStruct((chunks, n_ba, n_aa, kz_own, q_part, rows2, chans), BF),
        scratch_shapes=[
            vm((slots, n_y, depth, chans), BF),
            vm((2,) + weight_real.shape, BF),
            vm((2 * kz * stride, chans), F32),
            vm((halves, kz * 2 * ky * (n_x // halves), chans), F32),
            [rs_shape(t) for t in range(bits)], [rs_shape(t) for t in range(bits)],
            vm((chunks, n_aa, kz_own, q_part, rows2, chans), BF),
            vm((chunks, n_aa, kz_own, q_part, rows2, chans), BF),
            vm((n_ba, kz_own, ky_own, 2 * kx_own, chans), BF),
            vm((n_ba, kz_own, ky_own, 2 * kx_own, chans), BF),
            vm((n_ba, ky_own, kz_own, 2 * kx_own, chans), BF),
            vm((n_ba, ky_own, kz_own, 2 * kx_own, chans), BF),
            vm((chunks, n_aa, kz_own, q_part, rows2, chans), BF),
            dma((slots,)), dma((2, kx_own)),
            dma((bits, chunks)), dma((bits, chunks)),
            dma((chunks, n_aa)), dma((chunks, n_aa)),
            dma((2, n_ba)), dma((2, n_ba)),
            dma((chunks, n_aa)), dma((chunks, n_aa)),
            dma((bits, chunks)), dma((bits, chunks)),
        ],
        compiler_params=pltpu.CompilerParams(
            collective_id=0, has_side_effects=True, vmem_limit_bytes=67043328
        ),
    )(*tables, grid_features, weight_real, weight_imag)


def final_body(slots, table_ref, w_ref, bias_ref, back_ref, x_ref, out_ref, xbuf, obuf, in_sem, out_sem):
    n_x = x_ref.shape[0]
    n_y = x_ref.shape[1]
    c1 = 2.0 * math.sqrt(2.0 / math.pi)

    def fetch(i):
        return pltpu.make_async_copy(x_ref.at[i], xbuf.at[i % slots], in_sem.at[i % slots])

    def flush(i):
        return pltpu.make_async_copy(obuf.at[i % slots], out_ref.at[i], out_sem.at[i % slots])

    for i in range(slots):
        fetch(i).start()

    def step(i, carry):
        fetch(i).wait()

        @pl.when(i >= slots)
        def _():
            flush(i - slots).wait()

        slot = i % slots
        for j in range(n_y):
            lhs = jnp.concatenate([xbuf[slot, j], table_ref[...]], axis=1)
            rhs = jnp.concatenate([w_ref[...], back_ref[i, j], bias_ref[...]], axis=0)
            half = jnp.dot(lhs, rhs, preferred_element_type=F32)
            inner = half * (c1 + (4.0 * c1 * 0.044715) * (half * half))
            obuf[slot, j] = (half + half * jnp.tanh(inner)).astype(BF)
        flush(i).start()

        @pl.when(i + slots < n_x)
        def _():
            fetch(i + slots).start()

        return carry

    lax.fori_loop(0, n_x, step, 0)
    for i in range(n_x - slots, n_x):
        flush(i).wait()


def finish(grid_features, back, table, weight, bias):
    n_x, n_y, depth, chans = grid_features.shape
    modes = back.shape[2]
    extra = 16
    column = (np.arange(extra) == 0).astype(np.float32)
    table = np.concatenate([table.astype(np.float32), np.broadcast_to(column, (depth, extra))], axis=1)
    table = jnp.asarray((0.5 * table).astype(BF))
    weight = (0.5 * weight.astype(F32)).astype(BF)
    bias = (bias.astype(F32)[None, :] * column[:, None]).astype(BF)
    slots = 3
    inner = pl.BlockSpec(memory_space=pltpu.VMEM)
    outer = pl.BlockSpec(memory_space=pl.ANY)
    return pl.pallas_call(
        functools.partial(final_body, slots),
        in_specs=[inner] * 4 + [outer],
        out_specs=outer,
        out_shape=jax.ShapeDtypeStruct(grid_features.shape, BF),
        scratch_shapes=[
            pltpu.VMEM((slots, n_y, depth, chans), BF),
            pltpu.VMEM((slots, n_y, depth, chans), BF),
            pltpu.SemaphoreType.DMA((slots,)),
            pltpu.SemaphoreType.DMA((slots,)),
        ],
        compiler_params=pltpu.CompilerParams(vmem_limit_bytes=32 << 20),
        cost_estimate=pl.CostEstimate(
            flops=2 * n_x * n_y * depth * chans * (chans + modes),
            bytes_accessed=4 * n_x * n_y * depth * chans,
            transcendentals=n_x * n_y * depth * chans,
        ),
    )(table, weight, bias, back, grid_features)


def per_device(
    n_aa, n_ba, grid_features, weight_real, weight_imag, mode_keep, local_weight, local_bias
):
    n_x, n_y, depth, chans = grid_features.shape
    kx_own, ky, kz_own = weight_real.shape[:3]
    nx, ny = n_x * n_aa, n_y * n_ba
    kx, kz, ky_own = kx_own * n_ba, kz_own * n_aa, ky // n_ba
    bits = n_ba.bit_length() - 1
    me = lax.axis_index("ba")
    halves = max(n_x // 8, 1)
    parts = max(min(2, ky_own // 2), 1)
    x_half, q_part = n_x // halves, ky_own // parts

    c, s = phase_tables(depth, np.arange(depth), np.arange(kz))
    depth_fwd = np.concatenate([c, -s], axis=1).T.astype(BF)
    factor = np.where(np.arange(kz) == 0, 1.0, 2.0).astype(np.float32) / (nx * ny * depth)
    depth_inv = np.concatenate([c * factor, -s * factor], axis=1).astype(BF)

    y_fwd, y_inv = [], []
    order = np.arange(n_ba)
    block = np.zeros_like(order)
    for bit in range(bits):
        block = block + ((order >> (bits - 1 - bit)) & 1) * (1 << bit)
    for who in range(n_ba):
        ky_pos = ((block ^ who)[:, None] * ky_own + np.arange(ky_own)[None, :]).reshape(-1)
        ky_modes = kept_modes(ny, ky, ky_pos)
        own_y = who * n_y + np.arange(n_y)
        table = forward_table(ny, own_y, ky_modes)
        y_fwd.append(np.transpose(table, (3, 2, 0, 1)).reshape(2 * ky, 2 * n_y).astype(BF))
        y_inv.append(inverse_table(ny, own_y, ky_modes).astype(BF))
    y_fwd = jnp.asarray(np.stack(y_fwd))[me]
    y_inv = jnp.asarray(np.stack(y_inv))[me]
    x_modes = kept_modes(nx, kx, np.arange(kx))
    x_fwd = forward_table(nx, np.arange(nx), x_modes)
    x_fwd = x_fwd.reshape(2, n_aa, halves, x_half, 2, n_ba, kx_own)
    x_fwd = np.transpose(x_fwd, (5, 4, 6, 2, 1, 0, 3)).reshape(2 * kx, 2 * nx).astype(BF)
    x_inv = inverse_table(nx, np.arange(nx), x_modes)
    x_inv = x_inv.reshape(2, n_ba, kx_own, 2, n_aa, halves, x_half)
    x_inv = np.transpose(x_inv, (5, 4, 3, 6, 1, 0, 2)).reshape(2 * nx, 2 * kx).astype(BF)
    keep = jnp.concatenate([mode_keep.T, mode_keep.T], axis=1)
    keep = jnp.broadcast_to(keep[:, :, None], (kz_own, 2 * kx_own, chans))

    field = spectral(
        n_aa, n_ba, halves, parts, grid_features, weight_real, weight_imag,
        (depth_fwd, y_fwd, x_fwd, x_inv, keep),
    )
    field = field.reshape(halves, parts, n_ba, n_aa, kz_own, q_part, 2, x_half, chans)
    y_inv = y_inv.reshape(2, n_ba, parts, q_part, 2, n_y)
    back = jnp.einsum("hsbakqpxc,pbsqry->hxyrakc", field, y_inv, preferred_element_type=F32)
    back = back.astype(BF).reshape(n_x, n_y, 2 * kz, chans)
    return finish(grid_features, back, depth_inv, local_weight, local_bias)


def solution(mesh):
    in_specs = (
        P("aa", "ba", None, None),
        P("ba", None, "aa", None, None),
        P("ba", None, "aa", None, None),
        P("ba", "aa"),
        P(),
        P(),
    )
    out_specs = P("aa", "ba", None, None)
    body = functools.partial(per_device, mesh.shape["aa"], mesh.shape["ba"])
    return jax.shard_map(body, mesh=mesh, in_specs=in_specs, out_specs=out_specs, check_vma=False)
```

```python
import functools
import math

import jax
import jax.numpy as jnp
import numpy as np
from jax import lax
from jax.experimental import pallas as pl
from jax.experimental.pallas import tpu as pltpu
from jax.sharding import PartitionSpec as P

BF = jnp.bfloat16
F32 = jnp.float32
MESH = pl.DeviceIdType.MESH


def kept_modes(length, number, positions):
    return np.where(positions < number // 2, positions, positions + (length - number))


def phase_tables(length, places, mode_list):
    phase_steps = places[:, None] * mode_list[None, :] % length
    angles = phase_steps.astype(np.float32) * np.float32(2.0 * math.pi / length)
    return np.cos(angles), np.sin(angles)


def forward_table(length, places, modes):
    c, s = phase_tables(length, places, modes)
    return np.stack([np.stack([c, -s], 1), np.stack([s, c], 1)], 0)


def inverse_table(length, places, modes):
    c, s = phase_tables(length, places, modes)
    c, s = c.T, s.T
    return np.stack([np.stack([c, s], 1), np.stack([-s, c], 1)], 0)


def spectral_body(
    n_aa, n_ba, halves, parts, slots,
    depth_in, y_in, y_inv_in, x_fwd_in, x_inv_in, keep_in, x_ref, wr_ref, wi_ref,
    out_ref,
    depth_ref, y_ref, y_inv_ref, x_fwd_ref, x_inv_ref, keep_ref, kept_rows,
    xbuf, wbuf, lines, plane, sends, gots, outgo, landed, spec_out, spec_in,
    mix_out, mix_in, back, field,
    x_sem, w_sem, rs_send, rs_recv, fa_send, fa_recv, ba_send, ba_recv,
    ia_send, ia_recv, ag_send, ag_recv, o_sem, t_sem,
):
    n_x, n_y, depth, chans = x_ref.shape
    kx_own, ky, kz_own = wr_ref.shape[:3]
    kz = kz_own * n_aa
    ky_own = ky // n_ba
    q_part = ky_own // parts
    bits = n_ba.bit_length() - 1
    x_half = n_x // halves
    rows2 = 2 * x_half
    me_a = lax.axis_index("aa")
    me_b = lax.axis_index("ba")

    barrier = pltpu.get_barrier_semaphore()
    for d in range(1, n_aa):
        pl.semaphore_signal(barrier, inc=1, device_id=((me_a + d) % n_aa, me_b), device_id_type=MESH)
    for d in range(1, n_ba):
        pl.semaphore_signal(barrier, inc=1, device_id=(me_a, (me_b + d) % n_ba), device_id_type=MESH)

    def fetch(i):
        return pltpu.make_async_copy(x_ref.at[i], xbuf.at[i % slots], x_sem.at[i % slots])

    small = ((depth_in, depth_ref), (y_in, y_ref), (y_inv_in, y_inv_ref), (x_fwd_in, x_fwd_ref),
             (x_inv_in, x_inv_ref), (keep_in, keep_ref))
    tables = [pltpu.make_async_copy(src, dst, t_sem.at[n]) for n, (src, dst) in enumerate(small)]
    for copy in tables[:2]:
        copy.start()
    for i in range(slots):
        fetch(i).start()
    for copy in tables[2:]:
        copy.start()
    for copy in tables:
        copy.wait()
    own2 = 2 * kx_own
    place = lax.broadcasted_iota(jnp.int32, (own2, chans), 0) % kx_own
    for kk in range(kz_own):
        line = jnp.broadcast_to(keep_ref[kk : kk + 1, :].astype(F32), (own2, kx_own))
        spot = lax.broadcasted_iota(jnp.int32, (own2, kx_own), 0) % kx_own
        spot = spot == lax.broadcasted_iota(jnp.int32, (own2, kx_own), 1)
        kept_rows[kk] = jnp.broadcast_to(
            jnp.sum(jnp.where(spot, line, 0.0), axis=1, keepdims=True), (own2, chans)
        )

    stride = n_y + 8

    def depth_row(i, u2):
        fetch(i).wait()
        slot = i % slots
        for j in range(0, n_y, 2):
            pair = jnp.concatenate([xbuf[slot, j], xbuf[slot, j + 1]], axis=1)
            res = jnp.dot(depth_ref[...], pair, preferred_element_type=F32)
            for u in range(2):
                for g in range(2 * kz // 8):
                    lines[u2, pl.ds(8 * g * stride + j + u, 8, stride=stride), :] = res[
                        8 * g : 8 * g + 8, u * chans : (u + 1) * chans
                    ]

        @pl.when(i + slots < n_x)
        def _():
            fetch(i + slots).start()

    def y_row(i, u2):
        half = i // x_half
        local = i % x_half
        for k in range(0, kz, 2):
            cols = []
            for kk in (k, k + 1):
                re = lines[u2, kk * stride : kk * stride + n_y, :]
                im = lines[u2, (kz + kk) * stride : (kz + kk) * stride + n_y, :]
                cols.append(jnp.concatenate([re, im], axis=0).astype(BF))
            res = jnp.dot(y_ref[me_b], jnp.concatenate(cols, axis=1), preferred_element_type=F32)
            for u in range(2):
                for g in range(2 * ky // 8):
                    start = (k + u) * 2 * ky * x_half + 8 * g * x_half + local
                    plane[half, pl.ds(start, 8, stride=x_half), :] = res[
                        8 * g : 8 * g + 8, u * chans : (u + 1) * chans
                    ]

    def rows(t, carry):
        for u2 in range(2):
            depth_row(2 * t + u2, u2)
        for u2 in range(2):
            y_row(2 * t + u2, u2)
        return carry

    def partner(bit):
        return (me_a, me_b ^ (1 << bit))

    def chunk_sum(h, c, blk, k, q, upto):
        base = ((k * n_ba + blk) * parts + c) * q_part + q
        total = plane[h, pl.ds(base * rows2, rows2), :]
        for t in range(upto):
            total = total + gots[t][h * parts + c, blk, k, q].astype(F32)
        return total

    def rs_copy(s, g):
        return pltpu.make_async_remote_copy(
            src_ref=sends[s].at[g], dst_ref=gots[s].at[g],
            send_sem=rs_send.at[s, g], recv_sem=rs_recv.at[s, g],
            device_id=partner(s), device_id_type=MESH,
        )

    def rs_step(s, h, c):
        g = h * parts + c
        if s > 0:
            rs_copy(s - 1, g).wait_recv()
        left = n_ba >> (s + 1)

        def one(k, carry):
            for blk in range(left):
                for q in range(q_part):
                    sends[s][g, blk, k, q] = chunk_sum(h, c, left + blk, k, q, s).astype(BF)
            return carry

        lax.fori_loop(0, kz, one, 0)
        rs_copy(s, g).start()

    def fa_copy(g, d):
        peer = (me_a + d) % n_aa
        return pltpu.make_async_remote_copy(
            src_ref=outgo.at[g, peer], dst_ref=landed.at[g, me_a],
            send_sem=fa_send.at[g, d], recv_sem=fa_recv.at[g, d],
            device_id=(peer, me_b), device_id_type=MESH,
        )

    def fa_step(h, c):
        g = h * parts + c
        rs_copy(bits - 1, g).wait_recv()

        def one(a, carry):
            for kk in range(kz_own):
                for q in range(q_part):
                    outgo[g, a, kk, q] = chunk_sum(h, c, 0, a * kz_own + kk, q, bits).astype(BF)
            return carry

        lax.fori_loop(0, n_aa, one, 0)
        for d in range(1, n_aa):
            fa_copy(g, d).start()
        landed[g, me_a] = outgo[g, me_a]

    def weight_fetch(p, m):
        ref = (wr_ref, wi_ref)[p]
        return pltpu.make_async_copy(ref.at[m], wbuf.at[p, m], w_sem.at[p, m])

    steps_half = x_half // 2
    lax.fori_loop(0, steps_half, rows, 0)
    pl.semaphore_wait(barrier, n_aa + n_ba - 2)
    for c in range(parts):
        rs_step(0, 0, c)
    for h in range(1, halves):
        first = h * steps_half
        lax.fori_loop(first, first + 1, rows, 0)
        for c in range(parts):
            rs_step(1, h - 1, c)
        lax.fori_loop(first + 1, first + steps_half, rows, 0)
        for c in range(parts):
            rs_step(0, h, c)
    for p in range(2):
        for m in range(kx_own):
            weight_fetch(p, m).start()
    for c in range(parts):
        rs_step(1, halves - 1, c)
        for h in range(halves - 1):
            for s in range(2, bits):
                rs_step(s, h, c)
            fa_step(h, c)
    for c in range(parts):
        for s in range(2, bits):
            rs_step(s, halves - 1, c)
        fa_step(halves - 1, c)

    def ba_copy(which, c, d):
        peer = (me_b + d) % n_ba
        src, dst = ((spec_out, spec_in), (mix_out, mix_in))[which]
        return pltpu.make_async_remote_copy(
            src_ref=src.at[c, peer], dst_ref=dst.at[c, me_b],
            send_sem=ba_send.at[which, c, d], recv_sem=ba_recv.at[which, c, d],
            device_id=(me_a, peer), device_id_type=MESH,
        )

    def to_modes(c):
        for h in range(halves):
            for d in range(1, n_aa):
                fa_copy(h * parts + c, d).wait_recv()
        for kk in range(kz_own):
            for q in range(0, q_part, 2):
                cols = []
                for qq in (q, q + 1):
                    cols.append(jnp.concatenate(
                        [landed[h * parts + c, a, kk, qq] for h in range(halves) for a in range(n_aa)], axis=0
                    ))
                res = jnp.dot(x_fwd_ref[...], jnp.concatenate(cols, axis=1), preferred_element_type=F32)
                for u in range(2):
                    for b in range(n_ba):
                        spec_out[c, b, kk, q + u] = res[
                            b * own2 : (b + 1) * own2, u * chans : (u + 1) * chans
                        ].astype(BF)
        for d in range(1, n_ba):
            ba_copy(0, c, d).start()
        spec_in[c, me_b] = spec_out[c, me_b]

    def mix_modes(c):
        for d in range(1, n_ba):
            ba_copy(0, c, d).wait_recv()

        def mix(b, carry):
            for q in range(q_part):
                j = b * ky_own + c * q_part + q
                level = jnp.where(j < ky // 2, j, ky - 1 - j)
                for kk in range(kz_own):
                    val = spec_in[c, b, kk, q].astype(F32)
                    turned = jnp.concatenate([-val[kx_own:], val[:kx_own]], axis=0)
                    lhs = jnp.concatenate([val, turned], axis=1).astype(BF)
                    total = jnp.zeros((own2, chans), F32)
                    for m in range(0, kx_own, 2):
                        cols = [
                            jnp.concatenate([wbuf[0, mm, j, kk], wbuf[1, mm, j, kk]], axis=0)
                            for mm in (m, m + 1)
                        ]
                        res = jnp.dot(lhs, jnp.concatenate(cols, axis=1), preferred_element_type=F32)
                        total = jnp.where(place == m, res[:, :chans], total)
                        total = jnp.where(place == m + 1, res[:, chans:], total)
                    total = jnp.where(level.astype(F32) < kept_rows[kk], total, 0.0)
                    mix_out[c, b, q, kk] = total.astype(BF)
            return carry

        lax.fori_loop(0, n_ba, mix, 0)
        for d in range(1, n_ba):
            ba_copy(1, c, d).start()
        mix_in[c, me_b] = mix_out[c, me_b]

    def ia_copy(g, d):
        peer = (me_a + d) % n_aa
        return pltpu.make_async_remote_copy(
            src_ref=back.at[g, peer], dst_ref=field.at[g, 0, me_a],
            send_sem=ia_send.at[g, d], recv_sem=ia_recv.at[g, d],
            device_id=(peer, me_b), device_id_type=MESH,
        )

    def from_modes(c):
        for d in range(1, n_ba):
            ba_copy(1, c, d).wait_recv()
        for kk in range(kz_own):
            for q in range(0, q_part, 2):
                cols = []
                for qq in (q, q + 1):
                    cols.append(jnp.concatenate(
                        [mix_in[c, b, qq, kk].astype(F32) for b in range(n_ba)], axis=0
                    ).astype(BF))
                res = jnp.dot(x_inv_ref[...], jnp.concatenate(cols, axis=1), preferred_element_type=F32)
                for u in range(2):
                    for h in range(halves):
                        for a in range(n_aa):
                            first = (h * n_aa + a) * rows2
                            back[h * parts + c, a, kk, q + u] = res[
                                first : first + rows2, u * chans : (u + 1) * chans
                            ].astype(BF)

    def send_back(g):
        for d in range(1, n_aa):
            ia_copy(g, d).start()
        field[g, 0, me_a] = back[g, me_a]

    def ag_copy(t, g):
        n = 1 << (bits - 1 - t)
        return pltpu.make_async_remote_copy(
            src_ref=field.at[g, pl.ds(0, n)], dst_ref=field.at[g, pl.ds(n, n)],
            send_sem=ag_send.at[t, g], recv_sem=ag_recv.at[t, g],
            device_id=partner(t), device_id_type=MESH,
        )

    chunks = halves * parts
    steps = list(reversed(range(bits)))

    def gather_tick(tick):
        for n, t in enumerate(steps):
            g = tick - n
            if 0 <= g < chunks:
                if n == 0:
                    for d in range(1, n_aa):
                        ia_copy(g, d).wait_recv()
                else:
                    ag_copy(steps[n - 1], g).wait_recv()
                ag_copy(t, g).start()

    for tick in range(parts + 2):
        if tick < parts:
            to_modes(tick)
        if tick == 0:
            for p in range(2):
                for m in range(kx_own):
                    weight_fetch(p, m).wait()
        if 0 <= tick - 1 < parts:
            mix_modes(tick - 1)
        if 0 <= tick - 2 < parts:
            from_modes(tick - 2)
            send_back(tick - 2)
        if tick == parts + 1:
            for g in range(parts, chunks):
                send_back(g)
        if 0 <= tick - 4:
            gather_tick(tick - 4)
    ticks_done = max(parts + 2 - 4, 0)

    gap = kz + 8

    def spread(g):
        ag_copy(steps[-1], g).wait_recv()
        h, c = g // parts, g % parts

        def one(a, carry):
            for blk in range(n_ba):
                for kk in range(kz_own):
                    for q in range(q_part):
                        base = (((a * kz_own + kk) * n_ba + blk) * parts + c) * q_part + q
                        plane[h, pl.ds(base * rows2, rows2), :] = field[g, blk, a, kk, q].astype(F32)
            return carry

        lax.fori_loop(0, n_aa, one, 0)

    def flush(i):
        return pltpu.make_async_copy(
            xbuf.at[i % slots, :, pl.ds(0, 2 * kz)], out_ref.at[i], o_sem.at[i % slots]
        )

    def to_cells(i, carry):
        half = i // x_half
        local = i % x_half
        for k in range(0, kz, 2):
            cols = []
            for kk in (k, k + 1):
                first = kk * 2 * ky * x_half + local
                cols.append(jnp.concatenate(
                    [plane[half, pl.ds(first + 8 * g * x_half, 8, stride=x_half), :] for g in range(2 * ky // 8)],
                    axis=0,
                ).astype(BF))
            res = jnp.dot(y_inv_ref[me_b], jnp.concatenate(cols, axis=1), preferred_element_type=F32)
            for u in range(2):
                for g in range(2 * n_y // 8):
                    lines[0, pl.ds(8 * g * gap + k + u, 8, stride=gap), :] = res[
                        8 * g : 8 * g + 8, u * chans : (u + 1) * chans
                    ]

        @pl.when(i >= slots)
        def _():
            flush(i - slots).wait()

        for y in range(n_y):
            first = 2 * y * gap
            both = jnp.concatenate([lines[0, first : first + kz, :], lines[0, first + gap : first + gap + kz, :]], axis=0)
            xbuf[i % slots, y, 0 : 2 * kz, :] = both.astype(BF)
        flush(i).start()
        return carry

    cells_done = 0
    for tick in range(ticks_done, chunks + bits):
        gather_tick(tick)
        g = tick - bits
        if g >= 0:
            spread(g)
        ready = (g + 1) // parts * x_half
        upto = ready if tick == chunks + bits - 1 else min(ready, cells_done + 2)
        if upto > cells_done:
            lax.fori_loop(cells_done, upto, to_cells, 0)
            cells_done = upto
    for i in range(n_x - slots, n_x):
        flush(i).wait()

    for g in range(halves * parts):
        for s in range(bits):
            rs_copy(s, g).wait_send()
            ag_copy(s, g).wait_send()
        for d in range(1, n_aa):
            fa_copy(g, d).wait_send()
            ia_copy(g, d).wait_send()
    for which in range(2):
        for c in range(parts):
            for d in range(1, n_ba):
                ba_copy(which, c, d).wait_send()


def spectral(n_aa, n_ba, halves, parts, grid_features, weight_real, weight_imag, tables):
    n_x, n_y, depth, chans = grid_features.shape
    kx_own, ky, kz_own = weight_real.shape[:3]
    kz = kz_own * n_aa
    ky_own = ky // n_ba
    q_part = ky_own // parts
    bits = n_ba.bit_length() - 1
    rows2 = 2 * n_x // halves
    chunks = halves * parts
    slots = 4
    line_rows = max(2 * kz * (n_y + 8), 2 * n_y * (kz + 8))
    vm = pltpu.VMEM
    dma = pltpu.SemaphoreType.DMA

    def rs_shape(s):
        left = n_ba >> (s + 1)
        return vm((chunks, left, kz, q_part, rows2, chans), BF)

    outer = pl.BlockSpec(memory_space=pl.ANY)
    return pl.pallas_call(
        functools.partial(spectral_body, n_aa, n_ba, halves, parts, slots),
        in_specs=[outer] * 9,
        out_specs=outer,
        out_shape=jax.ShapeDtypeStruct((n_x, n_y, 2 * kz, chans), BF),
        scratch_shapes=[
            *[vm(t.shape, t.dtype) for t in tables],
            vm((kz_own, 2 * kx_own, chans), F32),
            vm((slots, n_y, depth, chans), BF),
            vm((2,) + weight_real.shape, BF),
            vm((2, line_rows, chans), F32),
            vm((halves, kz * 2 * ky * (n_x // halves), chans), F32),
            [rs_shape(t) for t in range(bits)], [rs_shape(t) for t in range(bits)],
            vm((chunks, n_aa, kz_own, q_part, rows2, chans), BF),
            vm((chunks, n_aa, kz_own, q_part, rows2, chans), BF),
            vm((parts, n_ba, kz_own, q_part, 2 * kx_own, chans), BF),
            vm((parts, n_ba, kz_own, q_part, 2 * kx_own, chans), BF),
            vm((parts, n_ba, q_part, kz_own, 2 * kx_own, chans), BF),
            vm((parts, n_ba, q_part, kz_own, 2 * kx_own, chans), BF),
            vm((chunks, n_aa, kz_own, q_part, rows2, chans), BF),
            vm((chunks, n_ba, n_aa, kz_own, q_part, rows2, chans), BF),
            dma((slots,)), dma((2, kx_own)),
            dma((bits, chunks)), dma((bits, chunks)),
            dma((chunks, n_aa)), dma((chunks, n_aa)),
            dma((2, parts, n_ba)), dma((2, parts, n_ba)),
            dma((chunks, n_aa)), dma((chunks, n_aa)),
            dma((bits, chunks)), dma((bits, chunks)), dma((slots,)), dma((len(tables),)),
        ],
        compiler_params=pltpu.CompilerParams(
            collective_id=0, has_side_effects=True, vmem_limit_bytes=67043328
        ),
    )(*tables, grid_features, weight_real, weight_imag)


def final_body(
    slots, table_in, w_in, bias_in, back_ref, x_ref, out_ref, table_ref, w_ref, bias_ref, xbuf, bbuf, obuf,
    w_half, bias_rows, in_sem, back_sem, out_sem, t_sem,
):
    n_x = x_ref.shape[0]
    n_y = x_ref.shape[1]
    c1 = 2.0 * math.sqrt(2.0 / math.pi)

    def fetch(i):
        return pltpu.make_async_copy(x_ref.at[i], xbuf.at[i % slots], in_sem.at[i % slots])

    def flush(i):
        return pltpu.make_async_copy(obuf.at[i % slots], out_ref.at[i], out_sem.at[i % slots])

    def fetch_back(i):
        return pltpu.make_async_copy(back_ref.at[i], bbuf.at[i % slots], back_sem.at[i % slots])

    small = ((table_in, table_ref), (w_in, w_ref), (bias_in, bias_ref))
    tables = [pltpu.make_async_copy(src, dst, t_sem.at[n]) for n, (src, dst) in enumerate(small)]
    for copy in tables:
        copy.start()
    for i in range(slots):
        fetch(i).start()
        fetch_back(i).start()
    for copy in tables:
        copy.wait()
    w_half[...] = (0.5 * w_ref[...].astype(F32)).astype(BF)
    bias_rows[...] = jnp.broadcast_to(bias_ref[...].astype(F32), bias_rows.shape).astype(BF)

    def step(i, carry):
        fetch(i).wait()
        fetch_back(i).wait()

        @pl.when(i >= slots)
        def _():
            flush(i - slots).wait()

        slot = i % slots
        for j in range(n_y):
            lhs = jnp.concatenate([xbuf[slot, j], table_ref[...]], axis=1)
            rhs = jnp.concatenate([w_half[...], bbuf[slot, j], bias_rows[...]], axis=0)
            half = jnp.dot(lhs, rhs, preferred_element_type=F32)
            inner = half * (c1 + (4.0 * c1 * 0.044715) * (half * half))
            obuf[slot, j] = (half + half * jnp.tanh(inner)).astype(BF)
        flush(i).start()

        @pl.when(i + slots < n_x)
        def _():
            fetch(i + slots).start()
            fetch_back(i + slots).start()

        return carry

    lax.fori_loop(0, n_x, step, 0)
    for i in range(n_x - slots, n_x):
        flush(i).wait()


def finish(grid_features, back, table, weight, bias):
    n_x, n_y, depth, chans = grid_features.shape
    modes = back.shape[2]
    extra = 16
    column = (np.arange(extra) == 0).astype(np.float32)
    table = np.concatenate([table.astype(np.float32), np.broadcast_to(column, (depth, extra))], axis=1)
    table = jnp.asarray((0.5 * table).astype(BF))
    slots = 3
    outer = pl.BlockSpec(memory_space=pl.ANY)
    return pl.pallas_call(
        functools.partial(final_body, slots),
        in_specs=[outer] * 5,
        out_specs=outer,
        out_shape=jax.ShapeDtypeStruct(grid_features.shape, BF),
        scratch_shapes=[
            pltpu.VMEM(table.shape, BF),
            pltpu.VMEM((chans, chans), BF),
            pltpu.VMEM((1, chans), BF),
            pltpu.VMEM((slots, n_y, depth, chans), BF),
            pltpu.VMEM((slots, n_y, modes, chans), BF),
            pltpu.VMEM((slots, n_y, depth, chans), BF),
            pltpu.VMEM((chans, chans), BF),
            pltpu.VMEM((extra, chans), BF),
            pltpu.SemaphoreType.DMA((slots,)),
            pltpu.SemaphoreType.DMA((slots,)),
            pltpu.SemaphoreType.DMA((slots,)),
            pltpu.SemaphoreType.DMA((3,)),
        ],
        compiler_params=pltpu.CompilerParams(vmem_limit_bytes=62 << 20),
        cost_estimate=pl.CostEstimate(
            flops=2 * n_x * n_y * depth * chans * (chans + modes),
            bytes_accessed=4 * n_x * n_y * depth * chans,
            transcendentals=n_x * n_y * depth * chans,
        ),
    )(table, weight, bias.reshape(1, chans), back, grid_features)


def per_device(
    n_aa, n_ba, grid_features, weight_real, weight_imag, mode_keep, local_weight, local_bias
):
    n_x, n_y, depth, chans = grid_features.shape
    kx_own, ky, kz_own = weight_real.shape[:3]
    nx, ny = n_x * n_aa, n_y * n_ba
    kx, kz, ky_own = kx_own * n_ba, kz_own * n_aa, ky // n_ba
    bits = n_ba.bit_length() - 1
    halves = max(n_x // 8, 1)
    parts = max(min(4, ky_own // 2), 1)
    x_half = n_x // halves

    c, s = phase_tables(depth, np.arange(depth), np.arange(kz))
    depth_fwd = np.concatenate([c, -s], axis=1).T.astype(BF)
    factor = np.where(np.arange(kz) == 0, 1.0, 2.0).astype(np.float32) / (nx * ny * depth)
    depth_inv = np.concatenate([c * factor, -s * factor], axis=1).astype(BF)

    y_fwd, y_inv = [], []
    order = np.arange(n_ba)
    block = np.zeros_like(order)
    for bit in range(bits):
        block = block + ((order >> (bits - 1 - bit)) & 1) * (1 << bit)
    for who in range(n_ba):
        ky_pos = ((block ^ who)[:, None] * ky_own + np.arange(ky_own)[None, :]).reshape(-1)
        ky_modes = kept_modes(ny, ky, ky_pos)
        own_y = who * n_y + np.arange(n_y)
        table = forward_table(ny, own_y, ky_modes)
        y_fwd.append(np.transpose(table, (3, 2, 0, 1)).reshape(2 * ky, 2 * n_y).astype(BF))
        table = inverse_table(ny, own_y, ky_modes)
        y_inv.append(np.transpose(table, (3, 2, 1, 0)).reshape(2 * n_y, 2 * ky).astype(BF))
    y_fwd, y_inv = np.stack(y_fwd), np.stack(y_inv)
    x_modes = kept_modes(nx, kx, np.arange(kx))
    x_fwd = forward_table(nx, np.arange(nx), x_modes)
    x_fwd = x_fwd.reshape(2, n_aa, halves, x_half, 2, n_ba, kx_own)
    x_fwd = np.transpose(x_fwd, (5, 4, 6, 2, 1, 0, 3)).reshape(2 * kx, 2 * nx).astype(BF)
    x_inv = inverse_table(nx, np.arange(nx), x_modes)
    x_inv = x_inv.reshape(2, n_ba, kx_own, 2, n_aa, halves, x_half)
    x_inv = np.transpose(x_inv, (5, 4, 3, 6, 1, 0, 2)).reshape(2 * nx, 2 * kx).astype(BF)
    back = spectral(
        n_aa, n_ba, halves, parts, grid_features, weight_real, weight_imag,
        (depth_fwd, y_fwd, y_inv, x_fwd, x_inv, mode_keep.T),
    )
    return finish(grid_features, back, depth_inv, local_weight, local_bias)


def solution(mesh):
    in_specs = (
        P("aa", "ba", None, None),
        P("ba", None, "aa", None, None),
        P("ba", None, "aa", None, None),
        P("ba", "aa"),
        P(),
        P(),
    )
    out_specs = P("aa", "ba", None, None)
    body = functools.partial(per_device, mesh.shape["aa"], mesh.shape["ba"])
    return jax.shard_map(body, mesh=mesh, in_specs=in_specs, out_specs=out_specs, check_vma=False)
```
